32 devices in a mesh: grp: 4 (over y, x), sub: 8 (over z, core).
Axes of the slice: x: 2, y: 2, z: 4, core: 2. Of those that a mesh axis runs over, the one named last changes fastest.
Arguments:
- initial_field: float32 [4, 16, 16384], P('grp', 'sub'), may hold values from -6 to 6
- conduct: float32 [4, 16, 16384], P('grp', 'sub'), may hold values from 0.02 to 0.12
- velocity: float32 [4, 16, 16384], P('grp', 'sub'), may hold values from 0 to 0.25
- heat_release: float32 [4, 16, 16384], P('grp', 'sub'), may hold values from 0.01 to 0.1
- group_kind: int32 [4], replicated, may hold values from 0 to 1, as said below
- partner: int32 [4], replicated, may hold values from 0 to 3, as said below
- surface_cell: int32 [4, 4096], P('grp', 'sub'), may hold values from 0 to 32767
- patch_count: int32 [4, 8], P('grp'), may hold values from 1 to 24, 64 in all within a row
- patch_centres: int32 [4, 192, 128], P('grp', 'sub'), may hold values from 0 to 4095, as said below
- patch_targets: int32 [4, 192, 128], P('grp', 'sub'), may hold values from 0 to 4095
- patch_maps: float32 [4, 192, 128, 128], P('grp', 'sub'), may hold values from -0.25 to 0.95
Outputs:
- temperature: float32 [4, 16, 16384], P('grp', 'sub')
- interface: float32 [4, 2, 4096], P('grp', None, 'sub')
The draws below stay inside these ranges and needn't reach their ends.
Inputs may be any that keep to these rules, and one draw needn't show every extreme that they name: `group_kind`: both kinds occur. partner[g] is a group of the other kind than g. Slots 0 to patch_count[g, j] - 1 of device j of group g are live; each group's counts sum to 64; in each group some device holds 24. `patch_centres`: the centres of slot s of group g lie in the cyclic window of 1024 consecutive nodes that starts at (s // 24) * 512 - 512 // 2 + h[g], for one shift h[g] of each group.
All inputs are finite; a program needn't handle non-finite values.
Results may differ from the reference program's by a relative error of at most 0.00013.
Values sent between devices are 32-bit elements; how exact they have to be, the bound alone decides.
A program may use at most 64 MiB of HBM per device.

```python
import math
import jax
import jax.numpy as jnp
import numpy as np
from jax import lax

PLANES = 2
CELLS = 16384
SURF_DEV = 512
PATCH = 128
STEPS = 4
COUPLE = 4
GROUPS = 4
STACK = 16
NODES = 4096
CAP = 24
SLOTS = 192
PATCH_ROW = 64
N_SUB = 8


def kinds_partners(key):
    base_key = jax.random.fold_in(key, 17)
    order_key, count_key, score_key = jax.random.split(base_key, 3)
    shuffled = jax.random.permutation(order_key, GROUPS)
    gas_count = jax.random.randint(count_key, (), 1, GROUPS)
    position = jnp.argsort(shuffled, stable=True)
    kinds = (position >= gas_count).astype(jnp.int32)
    scores = jax.random.randint(score_key, (GROUPS, GROUPS), 0, 1000) * GROUPS + jnp.arange(GROUPS)[None, :]
    scores = scores + (kinds[:, None] == kinds[None, :]).astype(jnp.int32) * 1000000
    partners = jnp.argsort(scores, axis=1, stable=True)[:, 0].astype(jnp.int32)
    return (kinds, partners)


def draw_group_kind(key, part):
    return kinds_partners(key)[0]


def draw_partner(key, part):
    return kinds_partners(key)[1]


def window_nodes(key, group_shift):
    owner = (jnp.arange(SLOTS, dtype=jnp.int32) // CAP)[None, :, None]
    start = owner * SURF_DEV - SURF_DEV // 2 + group_shift[:, None, None]
    offset = jax.random.randint(key, (GROUPS, SLOTS, PATCH), 0, 2 * SURF_DEV)
    return ((start + offset) % NODES).astype(jnp.int32)


def draw_patch_targets(key, part):
    target_key = jax.random.fold_in(key, 31)
    return jax.random.randint(target_key, (GROUPS, SLOTS, PATCH), 0, NODES).astype(jnp.int32)


def draw_patch_centres(key, part):
    centre_key = jax.random.fold_in(key, 47)
    shift_key, node_key = jax.random.split(centre_key)
    group_shift = jax.random.randint(shift_key, (GROUPS,), 0, NODES)
    return window_nodes(node_key, group_shift)


def draw_patch_maps(key, part):
    off_key, diag_key = jax.random.split(key)
    full_shape = (GROUPS, SLOTS, PATCH, PATCH)
    spread = jax.random.normal(off_key, full_shape, jnp.float32) * (0.5 / math.sqrt(PATCH))
    spread = jnp.clip(spread, -0.25, 0.25)
    diagonal = jax.random.uniform(diag_key, (GROUPS, SLOTS, PATCH), jnp.float32, 0.3, 0.7)
    return spread + diagonal[..., None] * jnp.eye(PATCH, dtype=jnp.float32)


def set_ends(result, own_key, low, top_value):
    longest = result.shape.index(max(result.shape))
    spots = []
    for shift in (0, 1):
        where = [jax.random.randint(jax.random.fold_in(own_key, axis), (), 0, length) for axis, length in enumerate(result.shape)]
        where[longest] = (where[longest] + shift) % result.shape[longest]
        spots.append(tuple(where))
    return result.at[spots[0]].set(low).at[spots[1]].set(top_value)


def steps_of(key, dims, cuts, low, high):
    loudness, own = 1.0, jax.random.fold_in(key, 6)
    for axis_at, shards_of in cuts:
        steps = jnp.exp(jax.random.uniform(jax.random.fold_in(own, axis_at), (shards_of,), jnp.float32, low / len(cuts), high / len(cuts)))
        loudness = loudness * jnp.repeat(steps, dims[axis_at] // shards_of).reshape([-1 if axis == axis_at else 1 for axis in range(len(dims))])
    return loudness


def length_profile(number_of, total, most, lean):
    weights = [(1 << 20) // math.isqrt(standing ** lean) + 1 for standing in range(2, number_of + 1)]
    spare, holding = total - most - (number_of - 1), [1] * (number_of - 1)
    while spare > 0:
        candidates = [i for i in range(number_of - 1) if holding[i] < most]
        whole, left = sum([weights[i] for i in candidates]), spare
        for i in candidates:
            addition = min(most - holding[i], max(1, left * weights[i] // whole), spare)
            holding[i] = holding[i] + addition
            spare = spare - addition
    return np.array([most] + holding)


def ragged(own_key, count, total, limit, slope):
    if count == 2:
        one = jax.random.randint(own_key, (), max(1, total - limit), min(limit, total - 1) + 1)
        return jnp.stack([one, total - one])
    sizes = jnp.asarray(length_profile(count, total, limit, slope), jnp.int32)
    pairs = (count - 1) // 2
    source_of, sink = sizes[1:1 + 2 * pairs:2], sizes[2:2 + 2 * pairs:2]
    room = jnp.minimum(source_of - 1, limit - sink)
    moved = jax.random.randint(jax.random.fold_in(own_key, 1), (pairs,), 0, 1 << 20) % (room + 1)
    sizes = sizes.at[1:1 + 2 * pairs:2].set(source_of - moved).at[2:2 + 2 * pairs:2].set(sink + moved)
    return sizes[jax.random.permutation(jax.random.fold_in(own_key, 2), count)]


def scatter_about(own_key, dims, deviation, reach, pieces=(), kind=jnp.bfloat16):
    result = deviation * jax.random.normal(own_key, dims, jnp.float32)
    if pieces:
        result = result * steps_of(own_key, dims, pieces, -0.22, 0.18)
    return jnp.clip(result, -reach, reach).astype(kind)


def setup_inputs(seed: int = 0) -> dict:
    key_list = jax.random.split(jax.random.key(seed), 12)
    initial_field = scatter_about(key_list[0], (GROUPS, STACK, CELLS), 1.0, 6.0, ((0, 4), (1, 8)), jnp.float32)
    conduct = jnp.clip(jnp.exp(math.log(0.12) - 1.7917595 * jax.random.uniform(key_list[1], (GROUPS, STACK, CELLS), jnp.float32) ** steps_of(key_list[1], (GROUPS, STACK, CELLS), ((0, 4), (1, 8)), -0.2, 0.2)), 0.02, 0.12)
    velocity = jnp.clip(0.25 * jax.random.uniform(key_list[2], (GROUPS, STACK, CELLS), jnp.float32) ** steps_of(key_list[2], (GROUPS, STACK, CELLS), ((0, 4), (1, 8)), -0.2, 0.2), 0.0, 0.25)
    heat_release = jnp.clip(jnp.exp(math.log(0.1) - 2.3025851 * jax.random.uniform(key_list[3], (GROUPS, STACK, CELLS), jnp.float32) ** steps_of(key_list[3], (GROUPS, STACK, CELLS), ((0, 4), (1, 8)), -0.2, 0.2)), 0.01, 0.1)
    group_kind = draw_group_kind(jax.random.fold_in(key_list[11], 71), 0)
    partner = draw_partner(jax.random.fold_in(key_list[11], 71), 0)
    surface_cell = set_ends(jax.random.randint(key_list[6], (GROUPS, NODES), 0, PLANES * CELLS), jax.random.fold_in(key_list[6], 1), 0, (PLANES * CELLS) - 1).astype(jnp.int32)
    patch_count = jax.vmap(lambda own: ragged(own, N_SUB, PATCH_ROW, CAP, 2))(jax.random.split(key_list[7], GROUPS)).reshape((GROUPS, N_SUB)).astype(jnp.int32)
    patch_centres = draw_patch_centres(jax.random.fold_in(key_list[11], 71), 0)
    patch_targets = draw_patch_targets(jax.random.fold_in(key_list[11], 71), 0)
    patch_maps = draw_patch_maps(jax.random.fold_in(key_list[11], 71), 0)
    return dict(initial_field=initial_field, conduct=conduct, velocity=velocity, heat_release=heat_release, group_kind=group_kind, partner=partner, surface_cell=surface_cell, patch_count=patch_count, patch_centres=patch_centres, patch_targets=patch_targets, patch_maps=patch_maps)


def in_plane(current):
    return (jnp.roll(current, 1, -2) + jnp.roll(current, -1, -2)
            + jnp.roll(current, 1, -1) + jnp.roll(current, -1, -1))


def advance(current, conduct, velocity, heat_release, gas_mask):
    zero_plane = jnp.zeros_like(current[:, :1])
    upper_plane = jnp.concatenate([current[:, 1:], zero_plane], axis=1)
    lower_plane = jnp.concatenate([zero_plane, current[:, :-1]], axis=1)
    laplace = upper_plane + lower_plane + in_plane(current) - 6.0 * current
    return (current + conduct * laplace - gas_mask * velocity * (current - lower_plane)
            + gas_mask * heat_release * jax.nn.sigmoid(2.0 * current))


def reference(initial_field, conduct, velocity, heat_release, group_kind, partner, surface_cell,
              patch_count, patch_centres, patch_targets, patch_maps):
    groups = initial_field.shape[0]
    slab_shape = (groups, N_SUB * PLANES, CELLS // 128, 128)
    current = initial_field.reshape(slab_shape)
    conduct_slab = conduct.reshape(slab_shape)
    velocity_slab = velocity.reshape(slab_shape)
    heat_slab = heat_release.reshape(slab_shape)
    gas_mask = (group_kind == 0).astype(jnp.float32)[:, None, None, None]
    gain_temp = jnp.where(group_kind == 0, 0.5, 0.25).astype(jnp.float32)[:, None]
    gain_flux = jnp.where(group_kind == 0, -0.25, 0.25).astype(jnp.float32)[:, None]
    node_ids = jnp.arange(N_SUB * SURF_DEV, dtype=jnp.int32)
    cell_ids = (node_ids // SURF_DEV)[None, :] * (PLANES * CELLS) + surface_cell
    slot_ids = jnp.arange(N_SUB * CAP, dtype=jnp.int32)
    live_mask = ((slot_ids % CAP)[None, :] < patch_count[:, slot_ids // CAP]).astype(jnp.float32)
    group_ids = jnp.arange(groups, dtype=jnp.int32)[:, None]
    interface = jnp.zeros((groups, 2, N_SUB * SURF_DEV), jnp.float32)
    for iteration in range(COUPLE):
        for substep in range(STEPS):
            current = advance(current, conduct_slab, velocity_slab, heat_slab, gas_mask)
        flux_field = conduct_slab * (4.0 * current - in_plane(current))
        flat_temp = current.reshape(groups, -1)
        flat_flux = flux_field.reshape(groups, -1)
        export = jnp.stack([jnp.take_along_axis(flat_temp, cell_ids, 1),
                            jnp.take_along_axis(flat_flux, cell_ids, 1)], axis=1)
        source = export[partner]
        row_sums = []
        for group in range(groups):
            centre_vals = source[group][:, patch_centres[group]]
            contrib = jnp.einsum("stk,qsk->qst", patch_maps[group], centre_vals,
                                 precision=lax.Precision.HIGHEST) * live_mask[group][None, :, None]
            row_sum = jnp.zeros((2, N_SUB * SURF_DEV), jnp.float32).at[:, patch_targets[group]].add(contrib)
            row_sums.append(row_sum)
        interface = jnp.stack(row_sums)
        increment = gain_temp * (interface[:, 0] - export[:, 0]) + gain_flux * interface[:, 1]
        flat_temp = flat_temp.at[group_ids, cell_ids].add(increment)
        current = flat_temp.reshape(slab_shape)
    return current.reshape(initial_field.shape), interface
```

```python
import jax
import jax.numpy as jnp
from jax import lax
from jax.experimental import pallas as pl
from jax.experimental.pallas import tpu as pltpu
from jax.sharding import PartitionSpec as P

STEPS = 4
COUPLE = 4
LANES = 128
F32 = jnp.float32
BF16 = jnp.bfloat16


def split(x):
    hi = x.astype(BF16).astype(F32)
    return hi, x - hi


def dot_nt(a, b):
    return lax.dot_general(a, b, (((1,), (1,)), ((), ())), preferred_element_type=F32)


def dot_nn(a, b):
    return lax.dot_general(a, b, (((1,), (0,)), ((), ())), preferred_element_type=F32)


def iota(shape, dim):
    return lax.broadcasted_iota(jnp.int32, shape, dim)


def in_plane(c):
    rows, cols = c.shape
    return (
        pltpu.roll(c, 1, 0)
        + pltpu.roll(c, rows - 1, 0)
        + pltpu.roll(c, 1, 1)
        + pltpu.roll(c, cols - 1, 1)
    )


def kernel(
    n,
    groups,
    kind_ref,
    partner_ref,
    count_ref,
    field_ref,
    cond_ref,
    vel_ref,
    heat_ref,
    surf_ref,
    cent_ref,
    targ_ref,
    maps_ref,
    out_ref,
    iface_ref,
    fa,
    fb,
    cx,
    vx,
    hx,
    land,
    surf_all,
    oh_surf,
    oh_cent,
    oh_targ,
    maps2,
    exp_buf,
    grp_land,
    sel_buf,
    gath,
    part,
    rs_land,
    inc_buf,
    inc_land,
    set_send,
    set_recv,
    grp_send,
    grp_recv,
    ga_send,
    ga_recv,
    rs_send,
    rs_recv,
    inc_send,
    inc_recv,
    halo_send,
    halo_recv,
):
    planes, rows, cols = field_ref.shape
    surf_here = surf_ref.shape[1]
    cap = cent_ref.shape[0]
    reach = -(-STEPS // planes)
    depth = reach * planes
    ext = planes + 2 * depth
    offs = [d for d in range(-reach, reach + 1) if d != 0]
    at = {d: i for i, d in enumerate(offs)}
    tile = 2 * surf_here // LANES
    half = surf_here // LANES
    me = lax.axis_index("sub")
    grp = lax.axis_index("grp")

    def there(d):
        return jnp.logical_and(me + d >= 0, me + d < n)

    def rcopy(src, dst, ss, rs, dev):
        return pltpu.make_async_remote_copy(
            src_ref=src,
            dst_ref=dst,
            send_sem=ss,
            recv_sem=rs,
            device_id=dev,
            device_id_type=pl.DeviceIdType.MESH,
        )

    for buf in (fa, cx, vx, hx):
        buf[...] = jnp.zeros(buf.shape, F32)
    land[...] = jnp.zeros(land.shape, F32)
    inc_land[...] = jnp.zeros(inc_land.shape, F32)
    surf_all[...] = jnp.zeros(surf_all.shape, jnp.int32)

    barrier = pltpu.get_barrier_semaphore()
    for k in range(1, n):
        pl.semaphore_signal(
            barrier, inc=1, device_id={"sub": lax.rem(me + k, n)}, device_id_type=pl.DeviceIdType.MESH
        )
    for k in range(1, groups):
        pl.semaphore_signal(
            barrier, inc=1, device_id={"grp": lax.rem(grp + k, groups)}, device_id_type=pl.DeviceIdType.MESH
        )
    pl.semaphore_wait(barrier, n - 1 + groups - 1)

    def coef_span(slot_d):
        base = depth + planes * slot_d
        return base, max(1, base) - base, min(ext - 1, base + planes) - base

    def setup_copies(to, slot):
        base, lo, hi = coef_span(slot)
        dev = {"sub": me + to}
        ss, rs = at[to], at[slot]
        pairs = [(field_ref, fa.at[pl.ds(base, planes)])]
        for src, dst in ((cond_ref, cx), (vel_ref, vx), (heat_ref, hx)):
            pairs.append((src.at[pl.ds(lo, hi - lo)], dst.at[pl.ds(base + lo, hi - lo)]))
        pairs.append((surf_ref, surf_all.at[slot + reach]))
        return [
            rcopy(s, t, set_send.at[j, ss], set_recv.at[j, rs], dev) for j, (s, t) in enumerate(pairs)
        ]

    for d in sorted(offs, key=abs):

        @pl.when(there(d))
        def _():
            for c in setup_copies(d, -d):
                c.start()

    kind = kind_ref[grp]
    gas = jnp.where(kind == 0, 1.0, 0.0).astype(F32)
    gain_t = jnp.where(kind == 0, 0.5, 0.25).astype(F32)
    gain_f = jnp.where(kind == 0, -0.25, 0.25).astype(F32)
    partner = partner_ref[grp]
    count = count_ref[0, me]
    own = pl.ds(depth, planes)
    fa[own] = field_ref[...]
    cx[own] = cond_ref[...]
    vx[own] = vel_ref[...]
    hx[own] = heat_ref[...]
    surf_all[reach] = surf_ref[...]
    node_row = iota((n * tile, LANES), 0)
    node_row = (node_row // tile) * half + node_row % half
    for s in range(cap):
        lanes = pl.ds(s * LANES, LANES)
        hit = (node_row == cent_ref[s : s + 1, :] // LANES).astype(F32).astype(BF16)
        oh_cent[pl.ds(0, n * tile), lanes] = hit
        oh_cent[pl.ds(n * tile, n * tile), lanes] = hit
        oh_targ[:, lanes] = (node_row == targ_ref[s : s + 1, :] // LANES).astype(F32).astype(BF16)
        live = jnp.where(s < count, 1.0, 0.0).astype(F32)
        hi, lo = split(maps_ref[s] * live)
        maps2[s, pl.ds(0, LANES)] = hi.astype(BF16)
        maps2[s, pl.ds(LANES, LANES)] = lo.astype(BF16)

    for d in offs:

        @pl.when(there(d))
        def _():
            for c in setup_copies(-d, d):
                c.wait_recv()
            for c in setup_copies(d, -d):
                c.wait_send()

    vx[...] = vx[...] * gas
    hx[...] = hx[...] * gas
    cell_row = iota((planes * rows, surf_here), 0)
    for j in range(2 * reach + 1):
        oh_surf[j] = (cell_row == surf_all[j] // LANES).astype(F32).astype(BF16)

    lane_of = iota((LANES, surf_here), 0)
    group_of_slots = 4 if cap % 4 == 0 else 1
    width = group_of_slots * LANES
    lane_of_chunk = iota((LANES, width), 0)
    q_of_row = iota((n * tile, LANES), 0) % tile >= half

    def step(src, dst, k):
        for z in range(k + 1, ext - k - 1):
            c = src[z]
            dn = src[z - 1]
            lap = src[z + 1] + dn + in_plane(c) - 6.0 * c
            dst[z] = c + cx[z] * lap - vx[z] * (c - dn) + hx[z] * jax.nn.sigmoid(2.0 * c)

    def as_row(t8):
        return jnp.concatenate([t8[i : i + 1, :] for i in range(half)], axis=1)

    def spread(slot, t8):
        hi, lo = split(as_row(t8))
        mine = lane_of == surf_all[slot] % LANES
        rhs = jnp.concatenate(
            [jnp.where(mine, hi, 0.0).astype(BF16), jnp.where(mine, lo, 0.0).astype(BF16)], axis=0
        )
        r = dot_nt(oh_surf[slot], rhs)
        return (r[:, :LANES] + r[:, LANES:]).reshape(planes, rows, LANES)

    def halo_copy(par, to, slot):
        return rcopy(
            fa.at[own],
            land.at[par, at[slot]],
            halo_send.at[par, at[to]],
            halo_recv.at[par, at[slot]],
            {"sub": me + to},
        )

    def inc_copy(to, slot):
        return rcopy(
            inc_buf, inc_land.at[at[slot]], inc_send.at[at[to]], inc_recv.at[at[slot]], {"sub": me + to}
        )

    def grp_copy(par, k):
        return rcopy(
            exp_buf,
            grp_land.at[par, k - 1],
            grp_send.at[par, k - 1],
            grp_recv.at[par, k - 1],
            {"grp": lax.rem(grp + k, groups)},
        )

    def gath_copy(k, sender):
        return rcopy(sel_buf, gath.at[sender], ga_send.at[k - 1], ga_recv.at[k - 1], {"sub": lax.rem(me + k, n)})

    def rs_copy(k, sender):
        peer = lax.rem(me + k, n)
        return rcopy(part.at[peer], rs_land.at[sender], rs_send.at[k - 1], rs_recv.at[k - 1], {"sub": peer})

    def couple(it, carry):
        par = lax.rem(it, 2)
        last = it == COUPLE - 1
        pair = (fa, fb)
        for k in range(STEPS):
            step(pair[k % 2], pair[(k + 1) % 2], k)
        final = pair[STEPS % 2]

        temp = jnp.concatenate([final[depth + p].T for p in range(planes)], axis=1)
        flux = jnp.concatenate(
            [
                (cx[depth + p] * (4.0 * final[depth + p] - in_plane(final[depth + p]))).T
                for p in range(planes)
            ],
            axis=1,
        )
        pieces = [x.astype(BF16) for v in (temp, flux) for x in split(v)]
        got = dot_nn(jnp.concatenate(pieces, axis=0), oh_surf[reach])
        mine = lane_of == surf_all[reach] % LANES
        for q in range(2):
            v = got[2 * q * LANES : (2 * q + 1) * LANES] + got[(2 * q + 1) * LANES : (2 * q + 2) * LANES]
            v = jnp.sum(jnp.where(mine, v, 0.0), axis=0, keepdims=True)
            for i in range(half):
                exp_buf[q * half + i : q * half + i + 1, :] = v[:, i * LANES : (i + 1) * LANES]

        for k in range(1, groups):
            grp_copy(par, k).start()
        for k in range(1, groups):
            grp_copy(par, k).wait_recv()
        sel = jnp.zeros((tile, LANES), F32)
        for k in range(1, groups):
            source = lax.rem(grp + groups - k, groups)
            sel = jnp.where(partner == source, grp_land[par, k - 1], sel)
        sel_buf[...] = sel
        for k in range(1, n):
            gath_copy(k, me).start()
        gath[me] = sel

        for d in offs:

            @pl.when(jnp.logical_and(there(d), jnp.logical_not(last)))
            def _():
                halo_copy(par, d, -d).start()

        for k in range(1, n):
            gath_copy(k, lax.rem(me + n - k, n)).wait_recv()

        src = gath[...].reshape(n * tile, LANES)
        both = jnp.concatenate([jnp.where(q_of_row, 0.0, src), jnp.where(q_of_row, src, 0.0)], axis=1)
        hi, lo = split(both)
        lhs = jnp.concatenate([hi, lo], axis=0).T.astype(BF16)
        acc = jnp.zeros((n * tile, 4 * LANES), F32)
        for s0 in range(0, cap, group_of_slots):
            lanes = slice(s0 * LANES, s0 * LANES + width)
            slots = range(s0, s0 + group_of_slots)
            cent = jnp.concatenate([cent_ref[s : s + 1, :] for s in slots], axis=1) % LANES
            vals = dot_nn(lhs, oh_cent[:, lanes])
            hit = lane_of_chunk == cent
            cv = [
                jnp.sum(jnp.where(hit, vals[q * LANES : (q + 1) * LANES], 0.0), axis=0, keepdims=True)
                for q in range(2)
            ]
            hi, lo = split(jnp.concatenate(cv, axis=0))
            c4 = jnp.concatenate([hi, lo], axis=0).astype(BF16)
            contrib = []
            for i, s in enumerate(slots):
                r = dot_nt(c4[:, i * LANES : (i + 1) * LANES], maps2[s])
                r = r[:, :LANES] + r[:, LANES:]
                contrib.append(r[0:2] + r[2:4])
            hi, lo = split(jnp.concatenate(contrib, axis=1))
            targ = jnp.concatenate([targ_ref[s : s + 1, :] for s in slots], axis=1) % LANES
            hit = lane_of_chunk == targ
            rhs = jnp.concatenate(
                [jnp.where(hit, x[q : q + 1], 0.0).astype(BF16) for q in range(2) for x in (hi, lo)], axis=0
            )
            acc = acc + dot_nt(oh_targ[:, lanes], rhs)
        p0 = acc[:, :LANES] + acc[:, LANES : 2 * LANES]
        p1 = acc[:, 2 * LANES : 3 * LANES] + acc[:, 3 * LANES :]
        part[...] = jnp.where(q_of_row, p1, p0).reshape(n, tile, LANES)
        for k in range(1, n):
            rs_copy(k, me).start()
        rs_land[me] = part[me]
        for k in range(1, n):
            rs_copy(k, lax.rem(me + n - k, n)).wait_recv()
        iface = rs_land[0]
        for j in range(1, n):
            iface = iface + rs_land[j]
        iface_ref[...] = iface
        inc = gain_t * (iface - exp_buf[...]) + pltpu.roll(gain_f * iface, half, 0)
        inc_buf[...] = inc
        for d in offs:

            @pl.when(jnp.logical_and(there(d), jnp.logical_not(last)))
            def _():
                inc_copy(d, -d).start()
                halo_copy(par, d, -d).wait_send()

        fa[own] = final[own] + spread(reach, inc)

        @pl.when(jnp.logical_not(last))
        def _():
            for d in offs:

                @pl.when(there(d))
                def _():
                    halo_copy(par, -d, d).wait_recv()
                    inc_copy(-d, d).wait_recv()

                fa[pl.ds(depth + planes * d, planes)] = land[par, at[d]] + spread(d + reach, inc_land[at[d]])
            for d in offs:

                @pl.when(there(d))
                def _():
                    inc_copy(d, -d).wait_send()

        for k in range(1, groups):
            grp_copy(par, k).wait_send()
        for k in range(1, n):
            gath_copy(k, me).wait_send()
            rs_copy(k, me).wait_send()
        return carry

    lax.fori_loop(0, COUPLE, couple, 0)
    out_ref[...] = fa[own]


def local_of(n, groups):
    def local(
        initial_field,
        conduct,
        velocity,
        heat_release,
        group_kind,
        partner,
        surface_cell,
        patch_count,
        patch_centres,
        patch_targets,
        patch_maps,
    ):
        _, planes, cells = initial_field.shape
        rows = cells // LANES
        slab = (planes, rows, LANES)
        surf_here = surface_cell.shape[1]
        cap = patch_centres.shape[1]
        reach = -(-STEPS // planes)
        ext = planes + 2 * reach * planes
        tile = 2 * surf_here // LANES
        vmem = pl.BlockSpec(memory_space=pltpu.VMEM)
        smem = pl.BlockSpec(memory_space=pltpu.SMEM)
        dma = pltpu.SemaphoreType.DMA
        nd = 2 * reach
        scratch = [
            pltpu.VMEM((ext, rows, LANES), F32),
            pltpu.VMEM((ext, rows, LANES), F32),
            pltpu.VMEM((ext, rows, LANES), F32),
            pltpu.VMEM((ext, rows, LANES), F32),
            pltpu.VMEM((ext, rows, LANES), F32),
            pltpu.VMEM((2, nd, planes, rows, LANES), F32),
            pltpu.VMEM((nd + 1, 1, surf_here), jnp.int32),
            pltpu.VMEM((nd + 1, planes * rows, surf_here), BF16),
            pltpu.VMEM((2 * n * tile, cap * LANES), BF16),
            pltpu.VMEM((n * tile, cap * LANES), BF16),
            pltpu.VMEM((cap, 2 * LANES, LANES), BF16),
            pltpu.VMEM((tile, LANES), F32),
            pltpu.VMEM((2, groups - 1, tile, LANES), F32),
            pltpu.VMEM((tile, LANES), F32),
            pltpu.VMEM((n, tile, LANES), F32),
            pltpu.VMEM((n, tile, LANES), F32),
            pltpu.VMEM((n, tile, LANES), F32),
            pltpu.VMEM((tile, LANES), F32),
            pltpu.VMEM((nd, tile, LANES), F32),
            dma((5, nd)),
            dma((5, nd)),
            dma((2, groups - 1)),
            dma((2, groups - 1)),
            dma((n - 1,)),
            dma((n - 1,)),
            dma((n - 1,)),
            dma((n - 1,)),
            dma((nd,)),
            dma((nd,)),
            dma((2, nd)),
            dma((2, nd)),
        ]

        def body(*refs):
            kernel(n, groups, *refs)

        field, iface = pl.pallas_call(
            body,
            name="coupled",
            out_shape=(
                jax.ShapeDtypeStruct(slab, F32),
                jax.ShapeDtypeStruct((tile, LANES), F32),
            ),
            in_specs=[smem] * 3 + [vmem] * 8,
            out_specs=(vmem, vmem),
            scratch_shapes=scratch,
            compiler_params=pltpu.CompilerParams(
                collective_id=0, has_side_effects=True, vmem_limit_bytes=56 * 1024 * 1024
            ),
        )(
            group_kind,
            partner,
            patch_count,
            initial_field.reshape(slab),
            conduct.reshape(slab),
            velocity.reshape(slab),
            heat_release.reshape(slab),
            surface_cell,
            patch_centres[0],
            patch_targets[0],
            patch_maps[0],
        )
        return field.reshape(initial_field.shape), iface.reshape(1, 2, surf_here)

    return local


def solution(mesh):
    placed = (
        P("grp", "sub", None),
        P("grp", "sub", None),
        P("grp", "sub", None),
        P("grp", "sub", None),
        P(),
        P(),
        P("grp", "sub"),
        P("grp", None),
        P("grp", "sub", None),
        P("grp", "sub", None),
        P("grp", "sub", None, None),
    )
    return jax.shard_map(
        local_of(mesh.shape["sub"], mesh.shape["grp"]),
        mesh=mesh,
        in_specs=placed,
        out_specs=(P("grp", "sub", None), P("grp", None, "sub")),
        check_vma=False,
    )
```

```python
import jax
import jax.numpy as jnp
from jax import lax
from jax.experimental import pallas as pl
from jax.experimental.pallas import tpu as pltpu
from jax.sharding import PartitionSpec as P

STEPS = 4
COUPLE = 4
LANES = 128
F32 = jnp.float32
BF16 = jnp.bfloat16


def split(x):
    hi = x.astype(BF16).astype(F32)
    return hi, x - hi


def dot_nt(a, b):
    return lax.dot_general(a, b, (((1,), (1,)), ((), ())), preferred_element_type=F32)


def dot_nn(a, b):
    return lax.dot_general(a, b, (((1,), (0,)), ((), ())), preferred_element_type=F32)


def iota(shape, dim):
    return lax.broadcasted_iota(jnp.int32, shape, dim)


def in_plane(c):
    rows, cols = c.shape
    return (
        pltpu.roll(c, 1, 0)
        + pltpu.roll(c, rows - 1, 0)
        + pltpu.roll(c, 1, 1)
        + pltpu.roll(c, cols - 1, 1)
    )


def kernel(
    n,
    groups,
    kind_ref,
    partner_ref,
    count_ref,
    field_ref,
    cond_ref,
    vel_ref,
    heat_ref,
    surf_ref,
    cent_ref,
    targ_ref,
    maps_ref,
    out_ref,
    iface_ref,
    fa,
    fb,
    cx,
    vx,
    hx,
    land,
    surf_all,
    oh_surf,
    oh_cent,
    oh_targ,
    maps2,
    exp_buf,
    grp_land,
    sel_buf,
    gath,
    part,
    rs_land,
    inc_buf,
    inc_land,
    set_send,
    set_recv,
    grp_send,
    grp_recv,
    ga_send,
    ga_recv,
    rs_send,
    rs_recv,
    inc_send,
    inc_recv,
    halo_send,
    halo_recv,
    maps,
    load_sem,
):
    planes = field_ref.shape[1]
    rows = fa.shape[1]
    near = STEPS // 2
    assert near % 2 == 0 and near <= planes
    surf_here = surf_ref.shape[1]
    cap = cent_ref.shape[0]
    reach = -(-STEPS // planes)
    depth = reach * planes
    ext = planes + 2 * depth
    offs = [d for d in range(-reach, reach + 1) if d != 0]
    at = {d: i for i, d in enumerate(offs)}
    tile = 2 * surf_here // LANES
    half = surf_here // LANES
    me = lax.axis_index("sub")
    grp = lax.axis_index("grp")

    def there(d):
        return jnp.logical_and(me + d >= 0, me + d < n)

    def rcopy(src, dst, ss, rs, dev):
        return pltpu.make_async_remote_copy(
            src_ref=src,
            dst_ref=dst,
            send_sem=ss,
            recv_sem=rs,
            device_id=dev,
            device_id_type=pl.DeviceIdType.MESH,
        )

    load = pltpu.make_async_copy(maps_ref, maps, load_sem)
    load.start()

    for buf in (fa, cx, vx, hx):
        buf[...] = jnp.zeros(buf.shape, F32)
    land[...] = jnp.zeros(land.shape, F32)
    inc_land[...] = jnp.zeros(inc_land.shape, F32)
    surf_all[...] = jnp.zeros(surf_all.shape, jnp.int32)

    barrier = pltpu.get_barrier_semaphore()
    for k in range(1, n):
        pl.semaphore_signal(
            barrier, inc=1, device_id={"sub": lax.rem(me + k, n)}, device_id_type=pl.DeviceIdType.MESH
        )
    for k in range(1, groups):
        pl.semaphore_signal(
            barrier, inc=1, device_id={"grp": lax.rem(grp + k, groups)}, device_id_type=pl.DeviceIdType.MESH
        )

    own = pl.ds(depth, planes)
    fetch = ((field_ref, fa), (cond_ref, cx), (vel_ref, vx), (heat_ref, hx))

    def unfold(b, carry):
        chunk = pl.ds(pl.multiple_of(b * 8 * LANES, LANES), 8 * LANES)
        for src, dst in fetch:
            x = src[0, :, chunk]
            for p in range(planes):
                dst[depth + p, pl.ds(pl.multiple_of(b * 8, 8), 8), :] = jnp.concatenate(
                    [x[p : p + 1, i * LANES : (i + 1) * LANES] for i in range(8)], axis=0
                )
        return carry

    lax.fori_loop(0, rows // 8, unfold, 0)
    pl.semaphore_wait(barrier, n - 1 + groups - 1)

    def send_planes(buf, lo, hi, to, j):
        slot = -to
        shift = depth - (depth + planes * slot)
        return rcopy(
            buf.at[pl.ds(lo + shift, hi - lo)],
            buf.at[pl.ds(lo, hi - lo)],
            set_send.at[j, at[to]],
            set_recv.at[j, at[slot]],
            {"sub": me + to},
        )

    def first_copies(to):
        base = depth - planes * to
        lo, hi = max(base, depth - near), min(base + planes, depth + planes + near)
        out = [send_planes(fa, lo, hi, to, 0)]
        lo, hi = max(base, depth - near + 1), min(base + planes, depth + planes + near - 1)
        if hi > lo:
            out += [send_planes(buf, lo, hi, to, j + 1) for j, buf in enumerate((cx, vx, hx))]
        return out

    def rest_copies(to, which):
        base = depth - planes * to
        lo, hi = max(base, 1), min(base + planes, ext - 1)
        if to == 1:
            hi = min(hi, depth - near + 1)
        if to == -1:
            lo = max(lo, depth + planes + near - 1)
        if hi <= lo:
            return []
        return [send_planes((cx, vx, hx)[j], lo, hi, to, j + 4) for j in which]

    def surf_copies(to):
        return [
            rcopy(
                surf_ref,
                surf_all.at[reach - to],
                set_send.at[7, at[to]],
                set_recv.at[7, at[-to]],
                {"sub": me + to},
            )
        ]

    def mid_copy(to):
        return rcopy(
            fa.at[own],
            land.at[1, at[-to]],
            set_send.at[8, at[to]],
            set_recv.at[8, at[-to]],
            {"sub": me + to},
        )

    def each(ds, act):
        for d in ds:

            @pl.when(there(d))
            def _():
                act(d)

    def starts(copies):
        for c in copies:
            c.start()

    def arrivals(copies):
        for c in copies:
            c.wait_recv()

    def departures(copies):
        for c in copies:
            c.wait_send()

    beside = (-1, 1)
    each(beside, lambda d: starts(first_copies(d)))

    kind = kind_ref[grp]
    gas = jnp.where(kind == 0, 1.0, 0.0).astype(F32)
    gain_t = jnp.where(kind == 0, 0.5, 0.25).astype(F32)
    gain_f = jnp.where(kind == 0, -0.25, 0.25).astype(F32)
    partner = partner_ref[grp]
    count = count_ref[0, me]
    surf_all[reach] = surf_ref[...]
    node_row = iota((n * tile, LANES), 0)
    node_row = (node_row // tile) * half + node_row % half
    load.wait()
    for s in range(cap):
        lanes = pl.ds(s * LANES, LANES)
        hit = (node_row == cent_ref[s : s + 1, :] // LANES).astype(F32).astype(BF16)
        oh_cent[pl.ds(0, n * tile), lanes] = hit
        oh_cent[pl.ds(n * tile, n * tile), lanes] = hit
        oh_targ[:, lanes] = (node_row == targ_ref[s : s + 1, :] // LANES).astype(F32).astype(BF16)
        live = jnp.where(s < count, 1.0, 0.0).astype(F32)
        hi, lo = split(maps[s] * live)
        maps2[s, pl.ds(0, LANES)] = hi.astype(BF16)
        maps2[s, pl.ds(LANES, LANES)] = lo.astype(BF16)

    cell_row = iota((planes * rows, surf_here), 0)

    def hot_rows(j):
        oh_surf[j] = (cell_row == surf_all[j] // LANES).astype(F32).astype(BF16)

    hot_rows(reach)

    lane_of = iota((LANES, surf_here), 0)
    group_of_slots = 4 if cap % 4 == 0 else 1
    width = group_of_slots * LANES
    lane_of_chunk = iota((LANES, width), 0)
    q_of_row = iota((n * tile, LANES), 0) % tile >= half

    def step(src, dst, k):
        for z in range(k + 1, ext - k - 1):
            c = src[z]
            dn = src[z - 1]
            lap = src[z + 1] + dn + in_plane(c) - 6.0 * c
            dst[z] = c + cx[z] * lap - gas * vx[z] * (c - dn) + gas * hx[z] * jax.nn.sigmoid(2.0 * c)

    def as_row(t8):
        return jnp.concatenate([t8[i : i + 1, :] for i in range(half)], axis=1)

    def spread(slot, t8):
        hi, lo = split(as_row(t8))
        mine = lane_of == surf_all[slot] % LANES
        rhs = jnp.concatenate(
            [jnp.where(mine, hi, 0.0).astype(BF16), jnp.where(mine, lo, 0.0).astype(BF16)], axis=0
        )
        r = dot_nt(oh_surf[slot], rhs)
        return (r[:, :LANES] + r[:, LANES:]).reshape(planes, rows, LANES)

    def halo_copy(par, to, slot):
        return rcopy(
            fa.at[own],
            land.at[par, at[slot]],
            halo_send.at[par, at[to]],
            halo_recv.at[par, at[slot]],
            {"sub": me + to},
        )

    def inc_copy(to, slot):
        return rcopy(
            inc_buf, inc_land.at[at[slot]], inc_send.at[at[to]], inc_recv.at[at[slot]], {"sub": me + to}
        )

    def grp_copy(par, k):
        return rcopy(
            exp_buf,
            grp_land.at[par, k - 1],
            grp_send.at[par, k - 1],
            grp_recv.at[par, k - 1],
            {"grp": lax.rem(grp + k, groups)},
        )

    def gath_copy(k, sender):
        return rcopy(sel_buf, gath.at[sender], ga_send.at[k - 1], ga_recv.at[k - 1], {"sub": lax.rem(me + k, n)})

    def rs_copy(k, sender):
        peer = lax.rem(me + k, n)
        return rcopy(part.at[peer], rs_land.at[sender], rs_send.at[k - 1], rs_recv.at[k - 1], {"sub": peer})

    def couple(it, carry):
        par = lax.rem(it, 2)
        last = it == COUPLE - 1
        first = it == 0
        final = fa

        @pl.when(jnp.logical_not(first))
        def _():
            for k in range(STEPS):
                step(pair[k % 2], pair[(k + 1) % 2], k)

        temp = jnp.concatenate([final[depth + p].T for p in range(planes)], axis=1)
        flux = jnp.concatenate(
            [
                (cx[depth + p] * (4.0 * final[depth + p] - in_plane(final[depth + p]))).T
                for p in range(planes)
            ],
            axis=1,
        )
        pieces = [x.astype(BF16) for v in (temp, flux) for x in split(v)]
        got = dot_nn(jnp.concatenate(pieces, axis=0), oh_surf[reach])
        mine = lane_of == surf_all[reach] % LANES
        for q in range(2):
            v = got[2 * q * LANES : (2 * q + 1) * LANES] + got[(2 * q + 1) * LANES : (2 * q + 2) * LANES]
            v = jnp.sum(jnp.where(mine, v, 0.0), axis=0, keepdims=True)
            for i in range(half):
                exp_buf[q * half + i : q * half + i + 1, :] = v[:, i * LANES : (i + 1) * LANES]

        for k in range(1, groups):
            grp_copy(par, k).start()
        for k in range(1, groups):
            grp_copy(par, k).wait_recv()
        sel = jnp.zeros((tile, LANES), F32)
        for k in range(1, groups):
            source = lax.rem(grp + groups - k, groups)
            sel = jnp.where(partner == source, grp_land[par, k - 1], sel)
        sel_buf[...] = sel
        for k in range(1, n):
            gath_copy(k, me).start()
        gath[me] = sel

        for d in offs:

            @pl.when(jnp.logical_and(there(d), jnp.logical_not(last)))
            def _():
                halo_copy(par, d, -d).start()

        for k in range(1, n):
            gath_copy(k, lax.rem(me + n - k, n)).wait_recv()

        src = gath[...].reshape(n * tile, LANES)
        both = jnp.concatenate([jnp.where(q_of_row, 0.0, src), jnp.where(q_of_row, src, 0.0)], axis=1)
        hi, lo = split(both)
        lhs = jnp.concatenate([hi, lo], axis=0).T.astype(BF16)
        acc = jnp.zeros((n * tile, 4 * LANES), F32)
        for s0 in range(0, cap, group_of_slots):
            lanes = slice(s0 * LANES, s0 * LANES + width)
            slots = range(s0, s0 + group_of_slots)
            cent = jnp.concatenate([cent_ref[s : s + 1, :] for s in slots], axis=1) % LANES
            vals = dot_nn(lhs, oh_cent[:, lanes])
            hit = lane_of_chunk == cent
            cv = [
                jnp.sum(jnp.where(hit, vals[q * LANES : (q + 1) * LANES], 0.0), axis=0, keepdims=True)
                for q in range(2)
            ]
            hi, lo = split(jnp.concatenate(cv, axis=0))
            c4 = jnp.concatenate([hi, lo], axis=0).astype(BF16)
            contrib = []
            for i, s in enumerate(slots):
                r = dot_nt(c4[:, i * LANES : (i + 1) * LANES], maps2[s])
                r = r[:, :LANES] + r[:, LANES:]
                contrib.append(r[0:2] + r[2:4])
            hi, lo = split(jnp.concatenate(contrib, axis=1))
            targ = jnp.concatenate([targ_ref[s : s + 1, :] for s in slots], axis=1) % LANES
            hit = lane_of_chunk == targ
            rhs = jnp.concatenate(
                [jnp.where(hit, x[q : q + 1], 0.0).astype(BF16) for q in range(2) for x in (hi, lo)], axis=0
            )
            acc = acc + dot_nt(oh_targ[:, lanes], rhs)
        p0 = acc[:, :LANES] + acc[:, LANES : 2 * LANES]
        p1 = acc[:, 2 * LANES : 3 * LANES] + acc[:, 3 * LANES :]
        part[...] = jnp.where(q_of_row, p1, p0).reshape(n, tile, LANES)
        for k in range(1, n):
            rs_copy(k, me).start()

        @pl.when(first)
        def _():
            each(offs, lambda d: starts(rest_copies(d, (2,))))

        rs_land[me] = part[me]
        for k in range(1, n):
            rs_copy(k, lax.rem(me + n - k, n)).wait_recv()
        iface = rs_land[0]
        for j in range(1, n):
            iface = iface + rs_land[j]
        for q in range(2):
            for i in range(half):
                iface_ref[0, q : q + 1, i * LANES : (i + 1) * LANES] = iface[q * half + i : q * half + i + 1, :]
        inc = gain_t * (iface - exp_buf[...]) + pltpu.roll(gain_f * iface, half, 0)
        inc_buf[...] = inc
        for d in offs:

            @pl.when(jnp.logical_and(there(d), jnp.logical_not(last)))
            def _():
                inc_copy(d, -d).start()
                halo_copy(par, d, -d).wait_send()

        @pl.when(first)
        def _():
            each(offs, lambda d: arrivals(surf_copies(-d)))
            for d in offs:
                hot_rows(d + reach)

        fa[own] = final[own] + spread(reach, inc)

        @pl.when(first)
        def _():
            each(offs, lambda d: arrivals(rest_copies(-d, (0, 1, 2))))
            each(offs, lambda d: departures(rest_copies(d, (0, 1, 2)) + surf_copies(d)))

        @pl.when(jnp.logical_not(last))
        def _():
            for d in offs:

                @pl.when(there(d))
                def _():
                    halo_copy(par, -d, d).wait_recv()
                    inc_copy(-d, d).wait_recv()

                fa[pl.ds(depth + planes * d, planes)] = land[par, at[d]] + spread(d + reach, inc_land[at[d]])
            for d in offs:

                @pl.when(there(d))
                def _():
                    inc_copy(d, -d).wait_send()

        for k in range(1, groups):
            grp_copy(par, k).wait_send()
        for k in range(1, n):
            gath_copy(k, me).wait_send()
            rs_copy(k, me).wait_send()
        return carry

    pair = (fa, fb)
    each(beside, lambda d: arrivals(first_copies(-d)))
    each(beside, lambda d: departures(first_copies(d)))
    for k in range(near):
        step(pair[k % 2], pair[(k + 1) % 2], depth - near + k)
    each(beside, lambda d: mid_copy(d).start())
    each(offs, lambda d: starts(surf_copies(d) + rest_copies(d, (0, 1))))
    each(beside, lambda d: mid_copy(-d).wait_recv())
    for d in beside:
        fa[pl.ds(depth + planes * d, planes)] = land[1, at[d]]
    each(beside, lambda d: mid_copy(d).wait_send())
    for k in range(near):
        step(pair[k % 2], pair[(k + 1) % 2], depth - near + k)

    lax.fori_loop(0, COUPLE, couple, 0)

    def fold(b, carry):
        chunk = pl.ds(pl.multiple_of(b * 8 * LANES, LANES), 8 * LANES)
        rws = []
        for p in range(planes):
            x = fa[depth + p, pl.ds(pl.multiple_of(b * 8, 8), 8), :]
            rws.append(jnp.concatenate([x[i : i + 1, :] for i in range(8)], axis=1))
        out_ref[0, :, chunk] = jnp.concatenate(rws, axis=0)
        return carry

    lax.fori_loop(0, rows // 8, fold, 0)


def local_of(n, groups):
    def local(
        initial_field,
        conduct,
        velocity,
        heat_release,
        group_kind,
        partner,
        surface_cell,
        patch_count,
        patch_centres,
        patch_targets,
        patch_maps,
    ):
        _, planes, cells = initial_field.shape
        rows = cells // LANES
        surf_here = surface_cell.shape[1]
        cap = patch_centres.shape[1]
        reach = -(-STEPS // planes)
        ext = planes + 2 * reach * planes
        tile = 2 * surf_here // LANES
        vmem = pl.BlockSpec(memory_space=pltpu.VMEM)
        smem = pl.BlockSpec(memory_space=pltpu.SMEM)
        dma = pltpu.SemaphoreType.DMA
        nd = 2 * reach
        scratch = [
            pltpu.VMEM((ext, rows, LANES), F32),
            pltpu.VMEM((ext, rows, LANES), F32),
            pltpu.VMEM((ext, rows, LANES), F32),
            pltpu.VMEM((ext, rows, LANES), F32),
            pltpu.VMEM((ext, rows, LANES), F32),
            pltpu.VMEM((2, nd, planes, rows, LANES), F32),
            pltpu.VMEM((nd + 1, 1, surf_here), jnp.int32),
            pltpu.VMEM((nd + 1, planes * rows, surf_here), BF16),
            pltpu.VMEM((2 * n * tile, cap * LANES), BF16),
            pltpu.VMEM((n * tile, cap * LANES), BF16),
            pltpu.VMEM((cap, 2 * LANES, LANES), BF16),
            pltpu.VMEM((tile, LANES), F32),
            pltpu.VMEM((2, groups - 1, tile, LANES), F32),
            pltpu.VMEM((tile, LANES), F32),
            pltpu.VMEM((n, tile, LANES), F32),
            pltpu.VMEM((n, tile, LANES), F32),
            pltpu.VMEM((n, tile, LANES), F32),
            pltpu.VMEM((tile, LANES), F32),
            pltpu.VMEM((nd, tile, LANES), F32),
            dma((9, nd)),
            dma((9, nd)),
            dma((2, groups - 1)),
            dma((2, groups - 1)),
            dma((n - 1,)),
            dma((n - 1,)),
            dma((n - 1,)),
            dma((n - 1,)),
            dma((nd,)),
            dma((nd,)),
            dma((2, nd)),
            dma((2, nd)),
            pltpu.VMEM((cap, LANES, LANES), F32),
            dma(()),
        ]

        def body(*refs):
            kernel(n, groups, *refs)

        field, iface = pl.pallas_call(
            body,
            name="coupled",
            out_shape=(
                jax.ShapeDtypeStruct(initial_field.shape, F32),
                jax.ShapeDtypeStruct((1, 2, surf_here), F32),
            ),
            in_specs=[smem] * 3 + [vmem] * 7 + [pl.BlockSpec(memory_space=pl.ANY)],
            out_specs=(vmem, vmem),
            scratch_shapes=scratch,
            compiler_params=pltpu.CompilerParams(
                collective_id=0, has_side_effects=True, vmem_limit_bytes=56 * 1024 * 1024
            ),
        )(
            group_kind,
            partner,
            patch_count,
            initial_field,
            conduct,
            velocity,
            heat_release,
            surface_cell,
            patch_centres[0],
            patch_targets[0],
            patch_maps[0],
        )
        return field, iface

    return local


def solution(mesh):
    placed = (
        P("grp", "sub", None),
        P("grp", "sub", None),
        P("grp", "sub", None),
        P("grp", "sub", None),
        P(),
        P(),
        P("grp", "sub"),
        P("grp", None),
        P("grp", "sub", None),
        P("grp", "sub", None),
        P("grp", "sub", None, None),
    )
    return jax.shard_map(
        local_of(mesh.shape["sub"], mesh.shape["grp"]),
        mesh=mesh,
        in_specs=placed,
        out_specs=(P("grp", "sub", None), P("grp", None, "sub")),
        check_vma=False,
    )
```
